32 devices in a mesh: section: 4 (over y, core), expert: 2 (over x), tensor: 4 (over z).
Axes of the slice: x: 2, y: 2, z: 4, core: 2. Of those that a mesh axis runs over, the one named last changes fastest.
Arguments:
- branch_weights: bfloat16 [2, 8192, 8192], P('expert', ('section', 'tensor')), may hold values from -0.125 to 0.125
- branch_gains: float32 [2, 8192], P('expert', ('section', 'tensor')), may hold values from 0.1 to 1.9
- column_order: int32 [2, 8192], P('expert'), may hold values from 0 to 8191, each once within a row
- layer_order: int32 [4], replicated, may hold values from 0 to 3, each once
- probe_seeds: int32 [1024], replicated, may hold values from 1 to 32767
Outputs:
- expert_weights: bfloat16 [2, 8192, 8192], P('expert', None, ('section', 'tensor'))
- checksum: float32 [2, 1024, 8192], P('expert', None, ('section', 'tensor'))
- fingerprint: float32 [2, 1024], P('expert')
- shared_gain: float32 [8192], replicated
The draws below stay inside these ranges and needn't reach their ends.
Inputs may be any that keep to these rules, and one draw needn't show every extreme that they name: Each row of column_order names every hidden unit once. layer_order names every layer once.
All inputs are finite; a program needn't handle non-finite values.
Results may differ from the reference program's by a relative error of at most 0.0034.
Values may be sent and summed in bfloat16 or wider, within the bound.
A program may use at most 64 MiB of HBM per device.

```python
import jax
import jax.numpy as jnp
from jax import lax

D = 2048
FF = 8192
LAYERS = 4
PROBES = 1024
EXPERTS = 2


def touch_ends(drawn, rng, least, top_value):
    index_at = [jax.random.randint(jax.random.fold_in(rng, axis), (), 0, length) for axis, length in enumerate(drawn.shape)]
    main_axis = drawn.shape.index(max(drawn.shape))
    beside = index_at[:main_axis] + [(index_at[main_axis] + 1) % drawn.shape[main_axis]] + index_at[main_axis + 1:]
    return drawn.at[tuple(index_at)].set(least).at[tuple(beside)].set(top_value)


def steps_of(key, shape, shards, least, top_value):
    factor_of = 1.0
    for dim, parts in shards:
        heights = jax.random.uniform(jax.random.fold_in(jax.random.fold_in(key, 6), dim), (parts,), jnp.float32, least / len(shards), top_value / len(shards))
        factor_of = factor_of * jnp.repeat(jnp.exp(heights), shape[dim] // parts).reshape((-1,) + (1,) * (len(shape) - 1 - dim))
    return factor_of


def scatter_about(key, dims, width, bound, split=(), kind=jnp.bfloat16):
    entries = width * jax.random.normal(key, dims, jnp.float32)
    if split:
        entries = entries * steps_of(key, dims, split, -0.22, 0.18)
    return jnp.clip(entries, -bound, bound).astype(kind)


def setup_inputs(seed: int = 0) -> dict:
    key_of = jax.random.split(jax.random.key(seed), 6)
    return {
        "branch_weights": scatter_about(key_of[0], (EXPERTS, LAYERS * D, FF), D ** -0.5, 0.125, ((0, 2), (1, 16))),
        "branch_gains": jnp.clip(1.0 + 0.18 * jax.random.normal(key_of[1], (EXPERTS, LAYERS * D), jnp.float32), 0.1, 1.9),
        "column_order": jax.vmap(lambda own: jax.random.permutation(own, FF))(jax.random.split(key_of[2], EXPERTS)).reshape((EXPERTS, FF)).astype(jnp.int32),
        "layer_order": jax.random.permutation(key_of[3], LAYERS).astype(jnp.int32),
        "probe_seeds": touch_ends(jax.random.randint(key_of[4], (PROBES,), 1, 32768), jax.random.fold_in(key_of[4], 1), 1, 32767).astype(jnp.int32),
    }


def probe_at(probe_seeds, row_ids):
    hashed = (probe_seeds[:, None] * (row_ids[None, :] + 1)) % 65521
    return ((hashed % 511) - 255).astype(jnp.float32) / 256.0


def reference(branch_weights, branch_gains, column_order, layer_order, probe_seeds):
    mean_gain = jnp.sum(branch_gains, axis=0) / EXPERTS
    slot_ids = jnp.arange(LAYERS, dtype=jnp.int32)
    inverse = jnp.sum(jnp.where(layer_order[None, :] == slot_ids[:, None], slot_ids[None, :], 0), axis=1).astype(jnp.int32)
    shared_gain = mean_gain.reshape(LAYERS, D)[inverse].reshape(LAYERS * D)
    probes = probe_at(probe_seeds, jnp.arange(LAYERS * D, dtype=jnp.int32)).astype(jnp.bfloat16)
    seven = jnp.full((1,), 7919, jnp.int32)
    column_probe = probe_at(seven, jnp.arange(FF, dtype=jnp.int32))[0]

    def one_expert(inputs):
        weights, own_gains, order = inputs
        permuted = jnp.take(weights, order, axis=1)
        scaling = own_gains / mean_gain
        folded = (permuted.astype(jnp.float32) * scaling[:, None]).astype(jnp.bfloat16)
        natural = folded.reshape(LAYERS, D, FF)[inverse].reshape(LAYERS * D, FF)
        sketches = jnp.dot(probes, natural, preferred_element_type=jnp.float32)
        printed = jnp.dot(sketches, column_probe, precision=lax.Precision.HIGHEST) * (FF ** -0.5)
        return natural, sketches, printed

    expert_weights, checksum, fingerprint = lax.map(one_expert, (branch_weights, branch_gains, column_order))
    return expert_weights, checksum, fingerprint, shared_gain
```

```python
import functools

import jax
import jax.numpy as jnp
from jax import lax
from jax.experimental import pallas as pl
from jax.experimental.pallas import tpu as pltpu
from jax.sharding import PartitionSpec as P

MESH = pl.DeviceIdType.MESH
LATE = 2


def probe_values(products):
    folded = (products >> 16) * 15 + (products & 65535)
    hashed = jnp.where(folded >= 65521, folded - 65521, folded)
    digits = (hashed >> 9) + (hashed & 511)
    digits = jnp.where(digits >= 511, digits - 511, digits)
    return (digits - 255).astype(jnp.float32) * (1.0 / 256.0)


def partner_of(n_section, n_tensor, section, tensor, k, sign):
    half = n_tensor // 2 if n_tensor % 2 == 0 else n_tensor
    sides = n_tensor // half
    m, cross = k // sides, (k + 1) % sides
    j = cross * (m // n_section % half) + (1 - cross) * ((m + 1) % half)
    q = cross * (m % n_section) + (1 - cross) * ((m + 1) // half % n_section)
    i = q if n_section % 2 else q % 2 * (n_section // 2) + q // 2
    t = ((tensor // half + cross) % sides) * half + (tensor % half + sign * j + half) % half
    return (section + sign * i + n_section) % n_section, t


def exchange(
    n_section, n_expert, n_tensor, layers, late,
    order_hbm, w_hbm, gains_hbm, cols_hbm, seeds_hbm,
    arrived, sums_ref, print_ref, means_ref, late_probes, order_ref,
    w, staged, acc, onehot, scale, print_acc, seed_col, probes, gains, parts,
    cols_ref, seeds_ref, order_s, own_scale, first_scale,
    w_sem, send_sem, recv_sem, gain_send, gain_recv, mean_send, mean_recv,
    part_send, part_recv, piece_send, piece_recv, scale_sem, small_sem,
):
    section, expert, tensor = (lax.axis_index(a) for a in ("section", "expert", "tensor"))
    groups = n_section * n_tensor
    me = section * n_tensor + tensor
    rows, width = w.shape
    cols = width // groups
    n_probes = seed_col.shape[0]
    n_tall, n_deep = w_sem.shape
    tall, deep = rows // n_tall, width // n_deep
    n_wide = piece_send.shape[0] // n_tall
    wide = cols // n_wide
    per_layer = groups // layers

    def partner(k, sign):
        return partner_of(n_section, n_tensor, section, tensor, k, sign)

    def remote(src, dst, send, recv, k):
        s, t = partner(k, 1)
        return pltpu.make_async_remote_copy(
            src_ref=src, dst_ref=dst, send_sem=send, recv_sem=recv,
            device_id={"section": s, "tensor": t}, device_id_type=MESH)

    def block_copy(k):
        s, t = partner(k, 1)
        return remote(
            staged.at[s * n_tensor + t], arrived.at[me], send_sem.at[k], recv_sem.at[k], k)

    def piece_copy(h, q):
        s, t = partner(0, 1)
        at = (slice(h * tall, (h + 1) * tall), slice(q * wide, (q + 1) * wide))
        return remote(
            staged.at[(s * n_tensor + t, *at)], arrived.at[(me, *at)],
            piece_send.at[h * n_wide + q], piece_recv.at[h * n_wide + q], 0)

    def scale_copy():
        return remote(own_scale, first_scale, scale_sem.at[0], scale_sem.at[1], 0)

    def mean_copy(k):
        return remote(means_ref.at[me], means_ref.at[me], mean_send.at[k], mean_recv.at[k], k)

    def part_copy(k):
        return remote(parts.at[me], parts.at[me], part_send.at[k], part_recv.at[k], k)

    def gain_copy(j):
        return pltpu.make_async_remote_copy(
            src_ref=gains.at[expert], dst_ref=gains.at[expert], send_sem=gain_send.at[j],
            recv_sem=gain_recv.at[j], device_id={"expert": (expert + j + 1) % n_expert},
            device_id_type=MESH)

    def w_copy(h, c):
        at = (pl.ds(h * tall, tall), pl.ds(pl.multiple_of(c * deep, deep), deep))
        return pltpu.make_async_copy(w_hbm.at[(0, *at)], w.at[at], w_sem.at[h, c])

    small = [
        pltpu.make_async_copy(src, dst, small_sem.at[i]) for i, (src, dst) in enumerate((
            (cols_hbm, cols_ref), (gains_hbm, gains.at[expert]), (seeds_hbm, seeds_ref),
            (order_hbm, order_s)))]
    for copy in small:
        copy.start()
    for h in range(n_tall):
        @pl.loop(0, n_deep)
        def _(c):
            w_copy(h, c).start()

    barrier = pltpu.get_barrier_semaphore()

    @pl.loop(0, n_expert - 1)
    def _(j):
        pl.semaphore_signal(
            barrier, inc=1, device_id={"expert": (expert + j + 1) % n_expert},
            device_id_type=MESH)

    @pl.loop(0, groups - 1)
    def _(k):
        s, t = partner(k, 1)
        pl.semaphore_signal(
            barrier, inc=1, device_id={"section": s, "tensor": t}, device_id_type=MESH)

    print_acc[...] = jnp.zeros_like(print_acc)
    small[0].wait()
    s0, t0 = partner(0, 1)
    g0 = s0 * n_tensor + t0

    for q in range(n_wide):
        wanted = cols_ref[:, pl.ds(pl.multiple_of(g0 * cols, cols) + q * wide, wide)]

        @pl.loop(0, n_deep)
        def _(c):
            ids = lax.broadcasted_iota(jnp.int32, (deep, wide), 0)
            onehot[pl.ds(pl.multiple_of(c * deep, deep), deep), :wide] = jnp.where(
                ids == wanted - c * deep, 1.0, 0.0).astype(jnp.bfloat16)

        for h in range(n_tall):
            part = (slice(h * tall, (h + 1) * tall), slice(q * wide, (q + 1) * wide))
            acc[part] = jnp.zeros((tall, wide), jnp.float32)

            @pl.loop(0, n_deep)
            def _(c):
                if q == 0:
                    w_copy(h, c).wait()
                at = pl.ds(pl.multiple_of(c * deep, deep), deep)
                acc[part] += jnp.dot(
                    w[part[0], at], onehot[at, :wide], preferred_element_type=jnp.float32)

            staged[(g0, *part)] = acc[part].astype(jnp.bfloat16)
            if q == 0 and h == 0:
                small[1].wait()
                pl.semaphore_wait(barrier, groups - 1 + n_expert - 1)

                @pl.loop(0, n_expert - 1)
                def _(j):
                    gain_copy(j).start()

            piece_copy(h, q).start()

    @pl.loop(0, n_expert - 1)
    def _(j):
        gain_copy(j).wait()

    total = gains[0]
    for e in range(1, n_expert):
        total = total + gains[e]
    mean = total / n_expert
    means_ref[me] = mean
    own_scale[...] = gains[expert] / mean
    scale[...] = jnp.broadcast_to(own_scale[...], (128, rows)).T
    scale_copy().start()

    @pl.loop(0, groups - 1)
    def _(k):
        mean_copy(k).start()

    def column_probe(g, c):
        ids = g * cols + c * 128 + lax.broadcasted_iota(jnp.int32, (1, 128), 1)
        return probe_values(7919 * (ids + 1))

    for c in range(cols // 128):
        part = slice(c * 128, (c + 1) * 128)
        block = (staged[g0, :, part].astype(jnp.float32) * scale[...]).astype(jnp.bfloat16)
        print_acc[...] += block.astype(jnp.float32) * column_probe(g0, c)

    @pl.loop(1, groups)
    def _(k):
        s, t = partner(k, 1)
        g = s * n_tensor + t
        wanted = cols_ref[:, pl.ds(pl.multiple_of(g * cols, cols), cols)]
        acc[...] = jnp.zeros_like(acc)

        @pl.loop(0, n_deep)
        def _(c):
            ids = lax.broadcasted_iota(jnp.int32, (deep, cols), 0)
            onehot[:deep] = jnp.where(ids == wanted - c * deep, 1.0, 0.0).astype(jnp.bfloat16)
            acc[...] += jnp.dot(
                w[:, pl.ds(pl.multiple_of(c * deep, deep), deep)], onehot[:deep],
                preferred_element_type=jnp.float32)

        for c in range(cols // 128):
            part = slice(c * 128, (c + 1) * 128)
            block = (acc[:, part] * scale[...]).astype(jnp.bfloat16)
            staged[g, :, part] = block
            print_acc[...] += block.astype(jnp.float32) * column_probe(g, c)

        @pl.when(k < groups - 2)
        def _():
            block_copy(k).start()

    small[2].wait()
    small[3].wait()
    sums_ref[...] = jnp.zeros_like(sums_ref)
    seeds = seeds_ref[...]
    seed_col[...] = jnp.broadcast_to(
        seeds.astype(jnp.float32), (128, n_probes)).T.astype(jnp.int32)
    for b in range(layers):
        order_ref[b:b + 1, :] = jnp.full((1, 128), order_s[0, b], jnp.int32).astype(jnp.float32)

    def first_row(g):
        return order_s[0, g // per_layer] * (rows * per_layer) + (g % per_layer) * rows

    totals = jnp.sum(print_acc[...], axis=1, keepdims=True)
    row_ids = first_row(me) + lax.broadcasted_iota(jnp.int32, (rows, 128), 0)
    for c in range(n_probes // 128):
        part = slice(c * 128, (c + 1) * 128)
        values = probe_values(seeds[:, part] * (row_ids + 1))
        parts[me, :, part] = jnp.sum(values * totals, axis=0, keepdims=True)

    @pl.loop(0, groups - 1)
    def _(k):
        part_copy(k).start()

    block_copy(groups - 2).start()

    def fill(k, to):
        s, t = partner(k, -1)
        first = first_row(s * n_tensor + t) + 1
        chunk = min(64, n_probes)

        @pl.loop(0, n_probes // chunk)
        def _(r):
            at = pl.ds(pl.multiple_of(r * chunk, chunk), chunk)
            for c in range(rows // 128):
                ids = first + c * 128 + lax.broadcasted_iota(jnp.int32, (1, 128), 1)
                to[at, c * 128:(c + 1) * 128] = probe_values(
                    seed_col[at, :] * ids).astype(jnp.bfloat16)

    def sketch(block):
        sums_ref[...] += jnp.dot(probes[...], block, preferred_element_type=jnp.float32)

    arrived[me] = staged[me]
    fill(groups - 1, probes)
    sketch(staged[me])

    fill(0, probes)
    scale_copy().wait()
    for i in range(n_tall * n_wide):
        piece_copy(i // n_wide, i % n_wide).wait()
    s0, t0 = partner(0, -1)
    first = s0 * n_tensor + t0
    scale[...] = jnp.broadcast_to(first_scale[...], (128, rows)).T
    for c in range(cols // 128):
        part = slice(c * 128, (c + 1) * 128)
        arrived[first, :, part] = (
            arrived[first, :, part].astype(jnp.float32) * scale[...]).astype(jnp.bfloat16)
    sketch(arrived[first])

    @pl.loop(1, groups - 1 - late)
    def _(k):
        s, t = partner(k, -1)
        fill(k, probes)
        block_copy(k).wait_recv()
        sketch(arrived[s * n_tensor + t])

    for j in range(late):
        fill(groups - 1 - late + j, late_probes.at[j])

    @pl.loop(0, groups - 1)
    def _(k):
        part_copy(k).wait()
        mean_copy(k).wait()

    printed = parts[0]
    for g in range(1, groups):
        printed = printed + parts[g]
    print_ref[...] = printed * width ** -0.5

    @pl.loop(groups - 1 - late, groups - 1)
    def _(k):
        block_copy(k).wait_recv()

    @pl.loop(1, groups - 1)
    def _(k):
        block_copy(k).wait_send()


def place(n_section, n_tensor, layers, late,
          order_ref, late_probes, blocks_ref, sums_ref, print_ref, means_ref,
          weights_out, sums_out, print_out, means_out,
          total, block_sem, mean_sem, sum_sem, print_sem):
    section, tensor = (lax.axis_index(a) for a in ("section", "tensor"))
    groups = blocks_ref.shape[0]
    per_layer = groups // layers
    chunk = sums_ref.shape[0] // sum_sem.shape[0]
    order = [jnp.max(order_ref[b:b + 1, :]).astype(jnp.int32) for b in range(layers)]

    def copies(g):
        to = order[g // per_layer] * per_layer + g % per_layer
        return (pltpu.make_async_copy(blocks_ref.at[g], weights_out.at[to], block_sem.at[g]),
                pltpu.make_async_copy(means_ref.at[g], means_out.at[to], mean_sem.at[g]))

    def sum_copy(r):
        at = pl.ds(r * chunk, chunk)
        return pltpu.make_async_copy(total.at[at], sums_out.at[at], sum_sem.at[r])

    print_copy = pltpu.make_async_copy(print_ref, print_out, print_sem)

    for g in range(groups):
        for copy in copies(g):
            copy.start()
    print_copy.start()

    for r in range(sum_sem.shape[0]):
        at = slice(r * chunk, (r + 1) * chunk)
        value = sums_ref[at, :]
        for j in range(late):
            s, t = partner_of(n_section, n_tensor, section, tensor, groups - 1 - late + j, -1)
            value += jnp.dot(late_probes[j, at, :], blocks_ref[s * n_tensor + t],
                             preferred_element_type=jnp.float32)
        total[at, :] = value
        sum_copy(r).start()

    for g in range(groups):
        for copy in copies(g):
            copy.wait()
    print_copy.wait()
    for r in range(sum_sem.shape[0]):
        sum_copy(r).wait()


def local(n_section, n_expert, n_tensor, branch_weights, branch_gains, column_order,
          layer_order, probe_seeds):
    _, rows, width = branch_weights.shape
    groups = n_section * n_tensor
    cols = width // groups
    layers = layer_order.shape[0]
    n_probes = probe_seeds.shape[0]
    deep = min(1024, width)
    late = min(LATE, groups - 2)
    n_tall = 2 if rows % 32 == 0 else 1
    n_wide = 2 if cols % 256 == 0 else 1
    f32, bf16 = jnp.float32, jnp.bfloat16
    vmem = pl.BlockSpec(memory_space=pltpu.VMEM)
    hbm = pl.BlockSpec(memory_space=pltpu.HBM)
    dma = pltpu.SemaphoreType.DMA
    arrived, sums, printed, means, late_probes, order = pl.pallas_call(
        functools.partial(exchange, n_section, n_expert, n_tensor, layers, late),
        out_shape=(
            jax.ShapeDtypeStruct((groups, rows, cols), bf16),
            jax.ShapeDtypeStruct((n_probes, cols), f32),
            jax.ShapeDtypeStruct((1, n_probes), f32),
            jax.ShapeDtypeStruct((groups, 1, rows), f32),
            jax.ShapeDtypeStruct((late, n_probes, rows), bf16),
            jax.ShapeDtypeStruct((-(-layers // 8) * 8, 128), f32),
        ),
        in_specs=[hbm] * 5,
        out_specs=(vmem,) * 6,
        scratch_shapes=[
            pltpu.VMEM((rows, width), bf16),
            pltpu.VMEM((groups, rows, cols), bf16),
            pltpu.VMEM((rows, cols), f32),
            pltpu.VMEM((width, cols), bf16),
            pltpu.VMEM((rows, 128), f32),
            pltpu.VMEM((rows, 128), f32),
            pltpu.VMEM((n_probes, 128), jnp.int32),
            pltpu.VMEM((n_probes, rows), bf16),
            pltpu.VMEM((n_expert, 1, rows), f32),
            pltpu.VMEM((groups, 1, n_probes), f32),
            pltpu.VMEM((1, width), jnp.int32),
            pltpu.VMEM((1, n_probes), jnp.int32),
            pltpu.SMEM((1, layers), jnp.int32),
            pltpu.VMEM((1, rows), f32),
            pltpu.VMEM((1, rows), f32),
            dma((n_tall, width // deep)), dma((groups,)), dma((groups,)),
            dma((n_expert,)), dma((n_expert,)), dma((groups,)), dma((groups,)),
            dma((groups,)), dma((groups,)), dma((n_tall * n_wide,)), dma((n_tall * n_wide,)),
            dma((2,)), dma((4,)),
        ],
        compiler_params=pltpu.CompilerParams(
            collective_id=0, has_side_effects=True, vmem_limit_bytes=40 * 2 ** 20),
        name="exchange",
    )(*(pltpu.with_memory_space_constraint(x, pltpu.HBM) for x in (
        layer_order.reshape(1, layers), branch_weights, branch_gains, column_order,
        probe_seeds.reshape(1, n_probes))))

    n_sums = 4 if n_probes % 512 == 0 else 1
    weights, sums, printed, means = pl.pallas_call(
        functools.partial(place, n_section, n_tensor, layers, late),
        in_specs=[vmem] * 6,
        out_specs=(hbm, hbm, hbm, hbm),
        scratch_shapes=[
            pltpu.VMEM((n_probes, cols), f32), dma((groups,)), dma((groups,)), dma((n_sums,)),
            dma(())],
        out_shape=(
            jax.ShapeDtypeStruct((groups, rows, cols), bf16),
            jax.ShapeDtypeStruct((n_probes, cols), f32),
            jax.ShapeDtypeStruct((1, n_probes), f32),
            jax.ShapeDtypeStruct((groups, 1, rows), f32),
        ),
        compiler_params=pltpu.CompilerParams(
            has_side_effects=True, vmem_limit_bytes=16 * 2 ** 20),
        name="place",
    )(order, late_probes, arrived, sums, printed, means)
    return (weights.reshape(1, groups * rows, cols), sums[None], printed,
            means.reshape(groups * rows))


def solution(mesh):
    sizes = mesh.shape
    return jax.shard_map(
        functools.partial(local, sizes["section"], sizes["expert"], sizes["tensor"]),
        mesh=mesh,
        in_specs=(
            P("expert", ("section", "tensor"), None),
            P("expert", ("section", "tensor")),
            P("expert", None),
            P(),
            P(),
        ),
        out_specs=(
            P("expert", None, ("section", "tensor")),
            P("expert", None, ("section", "tensor")),
            P("expert", None),
            P(),
        ),
        check_vma=False,
    )
```

```python
import functools

import jax
import jax.numpy as jnp
from jax import lax
from jax.experimental import pallas as pl
from jax.experimental.pallas import tpu as pltpu
from jax.sharding import PartitionSpec as P

MESH = pl.DeviceIdType.MESH
LATE = 1
HELD = 3


def probe_values(products):
    folded = (products >> 16) * 15 + (products & 65535)
    hashed = jnp.where(folded >= 65521, folded - 65521, folded)
    digits = (hashed >> 9) + (hashed & 511)
    digits = jnp.where(digits >= 511, digits - 511, digits)
    return (digits - 255).astype(jnp.float32) * (1.0 / 256.0)


def halves(n_tensor):
    half = n_tensor // 2 if n_tensor % 2 == 0 else n_tensor
    return half, n_tensor // half


def column_spans(cols):
    if cols % 512:
        return [(0, cols)]
    return [(0, cols // 4), (cols // 4, cols // 4), (cols // 2, cols // 2)]


def partner_of(n_section, n_tensor, section, tensor, k, sign):
    half, sides = halves(n_tensor)
    m, cross = k // sides, (k + 1) % sides
    j = cross * (m // n_section % half) + (1 - cross) * ((m + 1) % half)
    q = cross * (m % n_section) + (1 - cross) * ((m + 1) // half % n_section)
    i = q if n_section % 2 else q % 2 * (n_section // 2) + q // 2
    t = ((tensor // half + cross) % sides) * half + (tensor % half + sign * j + half) % half
    return (section + sign * i + n_section) % n_section, t


def exchange(
    n_section, n_expert, n_tensor, layers, late,
    order_hbm, w_hbm, gains_hbm, cols_hbm, seeds_hbm,
    arrived, sums_ref, print_ref, means_ref, late_probes, order_ref,
    w, staged, acc, onehot, scale, print_acc, seed_col, probes, gains, parts,
    own_part, cols_ref, seeds_ref, order_s, own_scale, first_scale,
    w_sem, send_sem, recv_sem, gain_send, gain_recv, mean_send, mean_recv,
    part_send, part_recv, print_send, print_recv, piece_send, piece_recv, scale_sem, small_sem,
):
    section, expert, tensor = (lax.axis_index(a) for a in ("section", "expert", "tensor"))
    groups = n_section * n_tensor
    me = section * n_tensor + tensor
    rows, width = w.shape
    cols = width // groups
    n_probes = seed_col.shape[0]
    n_tall, n_deep = w_sem.shape
    tall, deep = rows // n_tall, width // n_deep
    spans = column_spans(cols)
    per_layer = groups // layers
    half, sides = halves(n_tensor)
    near = n_section * half
    rank = section * half + tensor % half
    _, _, piece = parts.shape
    owners = n_probes // piece
    held = max(groups - 1 - HELD, 1)

    def partner(k, sign):
        return partner_of(n_section, n_tensor, section, tensor, k, sign)

    def remote(src, dst, send, recv, k):
        s, t = partner(k, 1)
        return pltpu.make_async_remote_copy(
            src_ref=src, dst_ref=dst, send_sem=send, recv_sem=recv,
            device_id={"section": s, "tensor": t}, device_id_type=MESH)

    def block_copy(k):
        s, t = partner(k, 1)
        return remote(
            staged.at[s * n_tensor + t], arrived.at[me], send_sem.at[k], recv_sem.at[k], k)

    def piece_copy(h, q):
        s, t = partner(0, 1)
        at = (pl.ds(h * tall, tall), pl.ds(*spans[q]))
        return remote(
            staged.at[(s * n_tensor + t, *at)], arrived.at[(me, *at)],
            piece_send.at[q * n_tall + h], piece_recv.at[q * n_tall + h], 0)

    def scale_copy():
        return remote(own_scale, first_scale, scale_sem.at[0], scale_sem.at[1], 0)

    def nearby(src, dst, send, recv, p):
        r = (rank + p) % near
        return pltpu.make_async_remote_copy(
            src_ref=src, dst_ref=dst, send_sem=send, recv_sem=recv,
            device_id={"section": r // half, "tensor": tensor // half * half + r % half},
            device_id_type=MESH)

    mirror = section * n_tensor + (tensor + half) % n_tensor

    def mirror_copy():
        return pltpu.make_async_remote_copy(
            src_ref=means_ref.at[me], dst_ref=means_ref.at[me], send_sem=mean_send.at[0],
            recv_sem=mean_recv.at[0], device_id={"tensor": (tensor + half) % n_tensor},
            device_id_type=MESH)

    def mean_copy(p):
        return nearby(means_ref.at[me], means_ref.at[me], mean_send.at[p], mean_recv.at[p], p)

    def relay_copy(p):
        return nearby(means_ref.at[mirror], means_ref.at[mirror],
                      mean_send.at[near + p], mean_recv.at[near + p], p)

    def owned(r):
        return pl.ds(pl.multiple_of(r * piece, piece), piece)

    def when_owner(r, act):
        if owners == near:
            act()
        else:
            pl.when(r < owners)(act)

    def part_copy(k):
        s, t = partner(k, 1)
        r = s * half + t % half
        return r, remote(own_part.at[:, owned(r % owners)], parts.at[me],
                         part_send.at[k], part_recv.at[k], k)

    def print_copy(p):
        at = owned(rank % owners)
        return nearby(print_ref.at[:, at], print_ref.at[:, at],
                      print_send.at[p], print_recv.at[p], p)

    def gain_copy(j):
        return pltpu.make_async_remote_copy(
            src_ref=gains.at[expert], dst_ref=gains.at[expert], send_sem=gain_send.at[j],
            recv_sem=gain_recv.at[j], device_id={"expert": (expert + j + 1) % n_expert},
            device_id_type=MESH)

    def w_copy(h, c):
        at = (pl.ds(h * tall, tall), pl.ds(pl.multiple_of(c * deep, deep), deep))
        return pltpu.make_async_copy(w_hbm.at[(0, *at)], w.at[at], w_sem.at[h, c])

    small = [
        pltpu.make_async_copy(src, dst, small_sem.at[i]) for i, (src, dst) in enumerate((
            (cols_hbm, cols_ref), (gains_hbm, gains.at[expert]), (seeds_hbm, seeds_ref),
            (order_hbm, order_s)))]
    for copy in small:
        copy.start()
    for h in range(n_tall):
        @pl.loop(0, n_deep)
        def _(c):
            w_copy(h, c).start()

    barrier = pltpu.get_barrier_semaphore()

    @pl.loop(0, n_expert - 1)
    def _(j):
        pl.semaphore_signal(
            barrier, inc=1, device_id={"expert": (expert + j + 1) % n_expert},
            device_id_type=MESH)

    @pl.loop(0, groups - 1)
    def _(k):
        s, t = partner(k, 1)
        pl.semaphore_signal(
            barrier, inc=1, device_id={"section": s, "tensor": t}, device_id_type=MESH)

    print_acc[...] = jnp.zeros_like(print_acc)
    small[0].wait()
    s0, t0 = partner(0, 1)
    g0 = s0 * n_tensor + t0

    for q, (left, wide) in enumerate(spans):
        wanted = cols_ref[:, pl.ds(pl.multiple_of(g0 * cols, cols) + left, wide)]

        @pl.loop(0, n_deep)
        def _(c):
            ids = lax.broadcasted_iota(jnp.int16, (deep, wide), 0)
            onehot[pl.ds(pl.multiple_of(c * deep, deep), deep), :wide] = jnp.where(
                ids == (wanted - c * deep).astype(jnp.int16), jnp.bfloat16(1), jnp.bfloat16(0))

        for h in range(n_tall):
            part = (slice(h * tall, (h + 1) * tall), slice(left, left + wide))
            acc[part] = jnp.zeros((tall, wide), jnp.float32)

            @pl.loop(0, n_deep)
            def _(c):
                if q == 0:
                    w_copy(h, c).wait()
                at = pl.ds(pl.multiple_of(c * deep, deep), deep)
                acc[part] += jnp.dot(
                    w[part[0], at], onehot[at, :wide], preferred_element_type=jnp.float32)

            staged[(g0, *part)] = acc[part].astype(jnp.bfloat16)
            if q == 0 and h == 0:
                small[1].wait()
                pl.semaphore_wait(barrier, groups - 1 + n_expert - 1)

                @pl.loop(0, n_expert - 1)
                def _(j):
                    gain_copy(j).start()

            piece_copy(h, q).start()

    @pl.loop(0, n_expert - 1)
    def _(j):
        gain_copy(j).wait()

    total = gains[0]
    for e in range(1, n_expert):
        total = total + gains[e]
    mean = total / n_expert
    means_ref[me] = mean
    own_scale[...] = gains[expert] / mean
    scale[...] = jnp.broadcast_to(own_scale[...], (128, rows)).T
    scale_copy().start()

    if sides == 2:
        mirror_copy().start()

    @pl.loop(1, near)
    def _(p):
        mean_copy(p).start()

    def column_probe(g, c):
        ids = g * cols + c * 128 + lax.broadcasted_iota(jnp.int32, (1, 128), 1)
        return probe_values(7919 * (ids + 1))

    for c in range(cols // 128):
        part = slice(c * 128, (c + 1) * 128)
        block = (staged[g0, :, part].astype(jnp.float32) * scale[...]).astype(jnp.bfloat16)
        print_acc[...] += block.astype(jnp.float32) * column_probe(g0, c)

    def permute(k):
        s, t = partner(k, 1)
        g = s * n_tensor + t
        wanted = cols_ref[:, pl.ds(pl.multiple_of(g * cols, cols), cols)]
        acc[...] = jnp.zeros_like(acc)

        @pl.loop(0, n_deep)
        def _(c):
            ids = lax.broadcasted_iota(jnp.int16, (deep, cols), 0)
            onehot[:deep] = jnp.where(
                ids == (wanted - c * deep).astype(jnp.int16), jnp.bfloat16(1), jnp.bfloat16(0))
            acc[...] += jnp.dot(
                w[:, pl.ds(pl.multiple_of(c * deep, deep), deep)], onehot[:deep],
                preferred_element_type=jnp.float32)

        for c in range(cols // 128):
            part = slice(c * 128, (c + 1) * 128)
            block = (acc[:, part] * scale[...]).astype(jnp.bfloat16)
            staged[g, :, part] = block
            print_acc[...] += block.astype(jnp.float32) * column_probe(g, c)

        @pl.when(k < held)
        def _():
            block_copy(k).start()

    @pl.loop(1, groups - 2)
    def _(n):
        permute(n + 2 - 4 * (n % 2) + 3 * ((groups - n) // (groups - 1)))

    @pl.loop(0, 2)
    def _(i):
        permute(groups - 3 + 2 * i)

    small[2].wait()
    small[3].wait()
    sums_ref[...] = jnp.zeros_like(sums_ref)
    seeds = seeds_ref[...]
    seed_col[...] = jnp.broadcast_to(
        seeds.astype(jnp.float32), (128, n_probes)).T.astype(jnp.int32)
    for b in range(layers):
        order_ref[b:b + 1, :] = jnp.full((1, 128), order_s[0, b], jnp.int32).astype(jnp.float32)

    def first_row(g):
        return order_s[0, g // per_layer] * (rows * per_layer) + (g % per_layer) * rows

    totals = jnp.sum(print_acc[...], axis=1, keepdims=True)
    row_ids = first_row(me) + lax.broadcasted_iota(jnp.int32, (rows, 128), 0)
    for c in range(n_probes // 128):
        part = slice(c * 128, (c + 1) * 128)
        values = probe_values(seeds[:, part] * (row_ids + 1))
        own_part[:, part] = jnp.sum(values * totals, axis=0, keepdims=True)

    @pl.loop(0, groups - 1)
    def _(k):
        r, copy = part_copy(k)
        when_owner(r, copy.start)

    if sides == 2:
        mirror_copy().wait()

        @pl.loop(1, near)
        def _(p):
            relay_copy(p).start()

    parts[me] = own_part[:, owned(rank % owners)]
    @pl.loop(held, groups - 1)
    def _(k):
        block_copy(k).start()

    def fill(k, to):
        s, t = partner(k, -1)
        first = first_row(s * n_tensor + t) + 1
        chunk = min(64, n_probes)

        @pl.loop(0, n_probes // chunk)
        def _(r):
            at = pl.ds(pl.multiple_of(r * chunk, chunk), chunk)
            for c in range(rows // 128):
                ids = first + c * 128 + lax.broadcasted_iota(jnp.int32, (1, 128), 1)
                to[at, c * 128:(c + 1) * 128] = probe_values(
                    seed_col[at, :] * ids).astype(jnp.bfloat16)

    def sketch(block):
        sums_ref[...] += jnp.dot(probes[...], block, preferred_element_type=jnp.float32)

    arrived[me] = staged[me]
    fill(groups - 1, probes)
    sketch(staged[me])

    fill(0, probes)
    scale_copy().wait()
    for i in range(n_tall * len(spans)):
        piece_copy(i % n_tall, i // n_tall).wait()
    s0, t0 = partner(0, -1)
    first = s0 * n_tensor + t0
    scale[...] = jnp.broadcast_to(first_scale[...], (128, rows)).T
    for c in range(cols // 128):
        part = slice(c * 128, (c + 1) * 128)
        arrived[first, :, part] = (
            arrived[first, :, part].astype(jnp.float32) * scale[...]).astype(jnp.bfloat16)
    sketch(arrived[first])

    def catch(k):
        s, t = partner(k, -1)
        fill(k, probes)
        block_copy(k).wait_recv()
        sketch(arrived[s * n_tensor + t])

    middle = max(min(held, groups - 1 - late), 1)
    pl.loop(1, middle)(catch)

    @pl.loop(0, groups - 1)
    def _(k):
        r, copy = part_copy(k)
        when_owner(r, copy.wait_send)

    def gather():
        @pl.loop(0, groups - 1)
        def _(k):
            part_copy(k)[1].wait_recv()

        printed = parts[0]
        for g in range(1, groups):
            printed = printed + parts[g]
        print_ref[:, owned(rank % owners)] = printed * width ** -0.5

        @pl.loop(1, near)
        def _(p):
            print_copy(p).start()

    when_owner(rank, gather)

    pl.loop(middle, groups - 1 - late)(catch)

    for j in range(late):
        fill(groups - 1 - late + j, late_probes.at[j])

    @pl.loop(1, near)
    def _(p):
        mean_copy(p).wait()
        if sides == 2:
            relay_copy(p).wait()
        when_owner((rank + near - p) % near, print_copy(p).wait_recv)
        when_owner(rank, print_copy(p).wait_send)

    @pl.loop(groups - 1 - late, groups - 1)
    def _(k):
        block_copy(k).wait_recv()

    @pl.loop(1, groups - 1)
    def _(k):
        block_copy(k).wait_send()


def place(n_section, n_tensor, layers, late,
          order_ref, late_probes, blocks_ref, sums_ref, print_ref, means_ref,
          weights_out, sums_out, print_out, means_out,
          total, block_sem, mean_sem, sum_sem, print_sem):
    section, tensor = (lax.axis_index(a) for a in ("section", "tensor"))
    groups = blocks_ref.shape[0]
    per_layer = groups // layers
    chunk = sums_ref.shape[0] // sum_sem.shape[0]
    order = [jnp.max(order_ref[b:b + 1, :]).astype(jnp.int32) for b in range(layers)]

    def copies(g):
        to = order[g // per_layer] * per_layer + g % per_layer
        return (pltpu.make_async_copy(blocks_ref.at[g], weights_out.at[to], block_sem.at[g]),
                pltpu.make_async_copy(means_ref.at[g], means_out.at[to], mean_sem.at[g]))

    def sum_copy(r):
        at = pl.ds(r * chunk, chunk)
        return pltpu.make_async_copy(total.at[at], sums_out.at[at], sum_sem.at[r])

    print_copy = pltpu.make_async_copy(print_ref, print_out, print_sem)

    for g in range(groups):
        for copy in copies(g):
            copy.start()
    print_copy.start()

    for r in range(sum_sem.shape[0]):
        at = slice(r * chunk, (r + 1) * chunk)
        value = sums_ref[at, :]
        for j in range(late):
            s, t = partner_of(n_section, n_tensor, section, tensor, groups - 1 - late + j, -1)
            value += jnp.dot(late_probes[j, at, :], blocks_ref[s * n_tensor + t],
                             preferred_element_type=jnp.float32)
        total[at, :] = value
        sum_copy(r).start()

    for g in range(groups):
        for copy in copies(g):
            copy.wait()
    print_copy.wait()
    for r in range(sum_sem.shape[0]):
        sum_copy(r).wait()


def local(n_section, n_expert, n_tensor, branch_weights, branch_gains, column_order,
          layer_order, probe_seeds):
    _, rows, width = branch_weights.shape
    groups = n_section * n_tensor
    cols = width // groups
    layers = layer_order.shape[0]
    n_probes = probe_seeds.shape[0]
    deep = min(1024, width)
    late = min(LATE, groups - 2)
    n_tall = 2 if rows % 32 == 0 else 1
    n_pieces = n_tall * len(column_spans(cols))
    near = n_section * halves(n_tensor)[0]
    owners = near if n_probes % (128 * near) == 0 else min(near, n_probes // 128)
    f32, bf16 = jnp.float32, jnp.bfloat16
    vmem = pl.BlockSpec(memory_space=pltpu.VMEM)
    hbm = pl.BlockSpec(memory_space=pltpu.HBM)
    dma = pltpu.SemaphoreType.DMA
    arrived, sums, printed, means, late_probes, order = pl.pallas_call(
        functools.partial(exchange, n_section, n_expert, n_tensor, layers, late),
        out_shape=(
            jax.ShapeDtypeStruct((groups, rows, cols), bf16),
            jax.ShapeDtypeStruct((n_probes, cols), f32),
            jax.ShapeDtypeStruct((1, n_probes), f32),
            jax.ShapeDtypeStruct((groups, 1, rows), f32),
            jax.ShapeDtypeStruct((late, n_probes, rows), bf16),
            jax.ShapeDtypeStruct((-(-layers // 8) * 8, 128), f32),
        ),
        in_specs=[hbm] * 5,
        out_specs=(vmem,) * 6,
        scratch_shapes=[
            pltpu.VMEM((rows, width), bf16),
            pltpu.VMEM((groups, rows, cols), bf16),
            pltpu.VMEM((rows, cols), f32),
            pltpu.VMEM((width, cols), bf16),
            pltpu.VMEM((rows, 128), f32),
            pltpu.VMEM((rows, 128), f32),
            pltpu.VMEM((n_probes, 128), jnp.int32),
            pltpu.VMEM((n_probes, rows), bf16),
            pltpu.VMEM((n_expert, 1, rows), f32),
            pltpu.VMEM((groups, 1, n_probes // owners), f32),
            pltpu.VMEM((1, n_probes), f32),
            pltpu.VMEM((1, width), jnp.int32),
            pltpu.VMEM((1, n_probes), jnp.int32),
            pltpu.SMEM((1, layers), jnp.int32),
            pltpu.VMEM((1, rows), f32),
            pltpu.VMEM((1, rows), f32),
            dma((n_tall, width // deep)), dma((groups,)), dma((groups,)),
            dma((n_expert,)), dma((n_expert,)), dma((2 * near,)), dma((2 * near,)),
            dma((groups,)), dma((groups,)), dma((near,)), dma((near,)),
            dma((n_pieces,)), dma((n_pieces,)), dma((2,)), dma((4,)),
        ],
        compiler_params=pltpu.CompilerParams(
            collective_id=0, has_side_effects=True, vmem_limit_bytes=40 * 2 ** 20),
        name="exchange",
    )(*(pltpu.with_memory_space_constraint(x, pltpu.HBM) for x in (
        layer_order.reshape(1, layers), branch_weights, branch_gains, column_order,
        probe_seeds.reshape(1, n_probes))))

    n_sums = 2 if n_probes % 512 == 0 else 1
    weights, sums, printed, means = pl.pallas_call(
        functools.partial(place, n_section, n_tensor, layers, late),
        in_specs=[vmem] * 6,
        out_specs=(hbm, hbm, hbm, hbm),
        scratch_shapes=[
            pltpu.VMEM((n_probes, cols), f32), dma((groups,)), dma((groups,)), dma((n_sums,)),
            dma(())],
        out_shape=(
            jax.ShapeDtypeStruct((groups, rows, cols), bf16),
            jax.ShapeDtypeStruct((n_probes, cols), f32),
            jax.ShapeDtypeStruct((1, n_probes), f32),
            jax.ShapeDtypeStruct((groups, 1, rows), f32),
        ),
        compiler_params=pltpu.CompilerParams(
            has_side_effects=True, vmem_limit_bytes=16 * 2 ** 20),
        name="place",
    )(order, late_probes, arrived, sums, printed, means)
    return (weights.reshape(1, groups * rows, cols), sums[None], printed,
            means.reshape(groups * rows))


def solution(mesh):
    sizes = mesh.shape
    return jax.shard_map(
        functools.partial(local, sizes["section"], sizes["expert"], sizes["tensor"]),
        mesh=mesh,
        in_specs=(
            P("expert", ("section", "tensor"), None),
            P("expert", ("section", "tensor")),
            P("expert", None),
            P(),
            P(),
        ),
        out_specs=(
            P("expert", None, ("section", "tensor")),
            P("expert", None, ("section", "tensor")),
            P("expert", None),
            P(),
        ),
        check_vma=False,
    )
```

```python
import functools

import jax
import jax.numpy as jnp
from jax import lax
from jax.experimental import pallas as pl
from jax.experimental.pallas import tpu as pltpu
from jax.sharding import PartitionSpec as P

MESH = pl.DeviceIdType.MESH
LATE = 1
HELD = 3


def probe_values(products):
    folded = (products >> 16) * 15 + (products & 65535)
    hashed = jnp.where(folded >= 65521, folded - 65521, folded)
    digits = (hashed >> 9) + (hashed & 511)
    digits = jnp.where(digits >= 511, digits - 511, digits)
    return (digits - 255).astype(jnp.float32) * (1.0 / 256.0)


def halves(n_tensor):
    half = n_tensor // 2 if n_tensor % 2 == 0 else n_tensor
    return half, n_tensor // half


def column_spans(cols):
    if cols % 512:
        return [(0, cols)]
    return [(0, cols // 4), (cols // 4, cols // 4), (cols // 2, cols // 2)]


def partner_of(n_section, n_tensor, section, tensor, k, sign):
    half, sides = halves(n_tensor)
    m, cross = k // sides, (k + 1) % sides
    j = cross * (m // n_section % half) + (1 - cross) * ((m + 1) % half)
    q = cross * (m % n_section) + (1 - cross) * ((m + 1) // half % n_section)
    i = q if n_section % 2 else q % 2 * (n_section // 2) + q // 2
    t = ((tensor // half + cross) % sides) * half + (tensor % half + sign * j + half) % half
    return (section + sign * i + n_section) % n_section, t


def exchange(
    n_section, n_expert, n_tensor, layers, late,
    order_hbm, w_hbm, gains_hbm, cols_hbm, seeds_hbm,
    arrived, sums_ref, print_ref, means_ref, late_probes, order_ref,
    w, staged, acc, onehot, scale, print_acc, seed_col, probes, gains, parts,
    own_part, cols_ref, seeds_ref, order_s, own_scale, first_scale,
    w_sem, send_sem, recv_sem, gain_send, gain_recv, mean_send, mean_recv,
    part_send, part_recv, print_send, print_recv, piece_send, piece_recv, scale_sem, small_sem,
):
    section, expert, tensor = (lax.axis_index(a) for a in ("section", "expert", "tensor"))
    groups = n_section * n_tensor
    me = section * n_tensor + tensor
    rows, width = w.shape
    cols = width // groups
    n_probes = seed_col.shape[0]
    n_tall, n_deep = w_sem.shape
    tall, deep = rows // n_tall, width // n_deep
    spans = column_spans(cols)
    per_layer = groups // layers
    half, sides = halves(n_tensor)
    near = n_section * half
    rank = section * half + tensor % half
    _, _, piece = parts.shape
    owners = n_probes // piece
    held = max(groups - 1 - HELD, 1)

    def partner(k, sign):
        return partner_of(n_section, n_tensor, section, tensor, k, sign)

    def remote(src, dst, send, recv, k):
        s, t = partner(k, 1)
        return pltpu.make_async_remote_copy(
            src_ref=src, dst_ref=dst, send_sem=send, recv_sem=recv,
            device_id={"section": s, "tensor": t}, device_id_type=MESH)

    def block_copy(k):
        s, t = partner(k, 1)
        return remote(
            staged.at[s * n_tensor + t], arrived.at[me], send_sem.at[k], recv_sem.at[k], k)

    def piece_copy(h, q):
        s, t = partner(0, 1)
        at = (pl.ds(h * tall, tall), pl.ds(*spans[q]))
        return remote(
            staged.at[(s * n_tensor + t, *at)], arrived.at[(me, *at)],
            piece_send.at[q * n_tall + h], piece_recv.at[q * n_tall + h], 0)

    def scale_copy():
        return remote(own_scale, first_scale, scale_sem.at[0], scale_sem.at[1], 0)

    def nearby(src, dst, send, recv, p):
        r = (rank + p) % near
        return pltpu.make_async_remote_copy(
            src_ref=src, dst_ref=dst, send_sem=send, recv_sem=recv,
            device_id={"section": r // half, "tensor": tensor // half * half + r % half},
            device_id_type=MESH)

    mirror = section * n_tensor + (tensor + half) % n_tensor

    def mirror_copy():
        return pltpu.make_async_remote_copy(
            src_ref=means_ref.at[me], dst_ref=means_ref.at[me], send_sem=mean_send.at[0],
            recv_sem=mean_recv.at[0], device_id={"tensor": (tensor + half) % n_tensor},
            device_id_type=MESH)

    def mean_copy(p):
        return nearby(means_ref.at[me], means_ref.at[me], mean_send.at[p], mean_recv.at[p], p)

    def relay_copy(p):
        return nearby(means_ref.at[mirror], means_ref.at[mirror],
                      mean_send.at[near + p], mean_recv.at[near + p], p)

    def owned(r):
        return pl.ds(pl.multiple_of(r * piece, piece), piece)

    def when_owner(r, act):
        if owners == near:
            act()
        else:
            pl.when(r < owners)(act)

    def part_copy(k):
        s, t = partner(k, 1)
        r = s * half + t % half
        return r, remote(own_part.at[:, owned(r % owners)], parts.at[me],
                         part_send.at[k], part_recv.at[k], k)

    def print_copy(p):
        at = owned(rank % owners)
        return nearby(print_ref.at[:, at], print_ref.at[:, at],
                      print_send.at[p], print_recv.at[p], p)

    def gain_copy(j):
        return pltpu.make_async_remote_copy(
            src_ref=gains.at[expert], dst_ref=gains.at[expert], send_sem=gain_send.at[j],
            recv_sem=gain_recv.at[j], device_id={"expert": (expert + j + 1) % n_expert},
            device_id_type=MESH)

    def w_copy(h, c):
        at = (pl.ds(h * tall, tall), pl.ds(pl.multiple_of(c * deep, deep), deep))
        return pltpu.make_async_copy(w_hbm.at[(0, *at)], w.at[at], w_sem.at[h, c])

    small = [
        pltpu.make_async_copy(src, dst, small_sem.at[i]) for i, (src, dst) in enumerate((
            (cols_hbm, cols_ref), (gains_hbm, gains.at[expert]), (seeds_hbm, seeds_ref),
            (order_hbm, order_s)))]
    for copy in small:
        copy.start()
    for h in range(n_tall):
        @pl.loop(0, n_deep)
        def _(c):
            w_copy(h, c).start()

    barrier = pltpu.get_barrier_semaphore()

    @pl.loop(0, n_expert - 1)
    def _(j):
        pl.semaphore_signal(
            barrier, inc=1, device_id={"expert": (expert + j + 1) % n_expert},
            device_id_type=MESH)

    @pl.loop(0, groups - 1)
    def _(k):
        s, t = partner(k, 1)
        pl.semaphore_signal(
            barrier, inc=1, device_id={"section": s, "tensor": t}, device_id_type=MESH)

    print_acc[...] = jnp.zeros_like(print_acc)
    small[0].wait()
    s0, t0 = partner(0, 1)
    g0 = s0 * n_tensor + t0

    for q, (left, wide) in enumerate(spans):
        wanted = cols_ref[:, pl.ds(pl.multiple_of(g0 * cols, cols) + left, wide)]

        @pl.loop(0, n_deep)
        def _(c):
            ids = lax.broadcasted_iota(jnp.int16, (deep, wide), 0)
            onehot[pl.ds(pl.multiple_of(c * deep, deep), deep), :wide] = jnp.where(
                ids == (wanted - c * deep).astype(jnp.int16), jnp.bfloat16(1), jnp.bfloat16(0))

        for h in range(n_tall):
            part = (slice(h * tall, (h + 1) * tall), slice(left, left + wide))
            acc[part] = jnp.zeros((tall, wide), jnp.float32)

            @pl.loop(0, n_deep)
            def _(c):
                if q == 0:
                    w_copy(h, c).wait()
                at = pl.ds(pl.multiple_of(c * deep, deep), deep)
                acc[part] += jnp.dot(
                    w[part[0], at], onehot[at, :wide], preferred_element_type=jnp.float32)

            staged[(g0, *part)] = acc[part].astype(jnp.bfloat16)
            if q == 0 and h == 0:
                small[1].wait()
                pl.semaphore_wait(barrier, groups - 1 + n_expert - 1)

                @pl.loop(0, n_expert - 1)
                def _(j):
                    gain_copy(j).start()

            piece_copy(h, q).start()

    @pl.loop(0, n_expert - 1)
    def _(j):
        gain_copy(j).wait()

    total = gains[0]
    for e in range(1, n_expert):
        total = total + gains[e]
    mean = total / n_expert
    means_ref[me] = mean
    own_scale[...] = gains[expert] / mean
    scale[...] = jnp.broadcast_to(own_scale[...], (128, rows)).T
    scale_copy().start()

    if sides == 2:
        mirror_copy().start()

    @pl.loop(1, near)
    def _(p):
        mean_copy(p).start()

    def column_probe(g, c):
        ids = g * cols + c * 128 + lax.broadcasted_iota(jnp.int32, (1, 128), 1)
        return probe_values(7919 * (ids + 1))

    for c in range(cols // 128):
        part = slice(c * 128, (c + 1) * 128)
        block = (staged[g0, :, part].astype(jnp.float32) * scale[...]).astype(jnp.bfloat16)
        print_acc[...] += block.astype(jnp.float32) * column_probe(g0, c)

    def permute(k):
        s, t = partner(k, 1)
        g = s * n_tensor + t
        wanted = cols_ref[:, pl.ds(pl.multiple_of(g * cols, cols), cols)]
        acc[...] = jnp.zeros_like(acc)

        @pl.loop(0, n_deep)
        def _(c):
            ids = lax.broadcasted_iota(jnp.int16, (deep, cols), 0)
            onehot[:deep] = jnp.where(
                ids == (wanted - c * deep).astype(jnp.int16), jnp.bfloat16(1), jnp.bfloat16(0))
            acc[...] += jnp.dot(
                w[:, pl.ds(pl.multiple_of(c * deep, deep), deep)], onehot[:deep],
                preferred_element_type=jnp.float32)

        for c in range(cols // 128):
            part = slice(c * 128, (c + 1) * 128)
            block = (acc[:, part] * scale[...]).astype(jnp.bfloat16)
            staged[g, :, part] = block
            print_acc[...] += block.astype(jnp.float32) * column_probe(g, c)

        @pl.when(k < held)
        def _():
            block_copy(k).start()

    @pl.loop(1, groups - 2)
    def _(n):
        permute(n + 2 - 4 * (n % 2) + 3 * ((groups - n) // (groups - 1)))

    @pl.loop(0, 2)
    def _(i):
        permute(groups - 3 + 2 * i)

    small[2].wait()
    small[3].wait()
    sums_ref[...] = jnp.zeros_like(sums_ref)
    seeds = seeds_ref[...]
    seed_col[...] = jnp.broadcast_to(
        seeds.astype(jnp.float32), (128, n_probes)).T.astype(jnp.int32)
    for b in range(layers):
        order_ref[b:b + 1, :] = jnp.full((1, 128), order_s[0, b], jnp.int32).astype(jnp.float32)

    def first_row(g):
        return order_s[0, g // per_layer] * (rows * per_layer) + (g % per_layer) * rows

    totals = jnp.sum(print_acc[...], axis=1, keepdims=True)
    row_ids = first_row(me) + lax.broadcasted_iota(jnp.int32, (rows, 128), 0)
    for c in range(n_probes // 128):
        part = slice(c * 128, (c + 1) * 128)
        values = probe_values(seeds[:, part] * (row_ids + 1))
        own_part[:, part] = jnp.sum(values * totals, axis=0, keepdims=True)

    @pl.loop(0, groups - 1)
    def _(k):
        r, copy = part_copy(k)
        when_owner(r, copy.start)

    if sides == 2:
        mirror_copy().wait()

        @pl.loop(1, near)
        def _(p):
            relay_copy(p).start()

    parts[me] = own_part[:, owned(rank % owners)]
    @pl.loop(held, groups - 1)
    def _(k):
        block_copy(k).start()

    def fill(k, to):
        s, t = partner(k, -1)
        first = first_row(s * n_tensor + t) + 1
        chunk = min(64, n_probes)

        @pl.loop(0, n_probes // chunk)
        def _(r):
            at = pl.ds(pl.multiple_of(r * chunk, chunk), chunk)
            for c in range(rows // 128):
                ids = first + c * 128 + lax.broadcasted_iota(jnp.int32, (1, 128), 1)
                to[at, c * 128:(c + 1) * 128] = probe_values(
                    seed_col[at, :] * ids).astype(jnp.bfloat16)

    def sketch(block):
        sums_ref[...] += jnp.dot(probes[...], block, preferred_element_type=jnp.float32)

    arrived[me] = staged[me]
    fill(groups - 1, probes)
    sketch(staged[me])

    fill(0, probes)
    scale_copy().wait()
    for i in range(n_tall * len(spans)):
        piece_copy(i % n_tall, i // n_tall).wait()
    s0, t0 = partner(0, -1)
    first = s0 * n_tensor + t0
    scale[...] = jnp.broadcast_to(first_scale[...], (128, rows)).T
    for c in range(cols // 128):
        part = slice(c * 128, (c + 1) * 128)
        arrived[first, :, part] = (
            arrived[first, :, part].astype(jnp.float32) * scale[...]).astype(jnp.bfloat16)
    sketch(arrived[first])

    def catch(k):
        s, t = partner(k, -1)
        fill(k, probes)
        block_copy(k).wait_recv()
        sketch(arrived[s * n_tensor + t])

    middle = max(min(held, groups - 1 - late), 1)
    pl.loop(1, middle)(catch)

    @pl.loop(0, groups - 1)
    def _(k):
        r, copy = part_copy(k)
        when_owner(r, copy.wait_send)

    def gather():
        @pl.loop(0, groups - 1)
        def _(k):
            part_copy(k)[1].wait_recv()

        printed = parts[0]
        for g in range(1, groups):
            printed = printed + parts[g]
        print_ref[:, owned(rank % owners)] = printed * width ** -0.5

        @pl.loop(1, near)
        def _(p):
            print_copy(p).start()

    when_owner(rank, gather)

    pl.loop(middle, groups - 1 - late)(catch)

    for j in range(late):
        fill(groups - 1 - late + j, late_probes.at[j])

    @pl.loop(1, near)
    def _(p):
        mean_copy(p).wait()
        if sides == 2:
            relay_copy(p).wait()
        when_owner((rank + near - p) % near, print_copy(p).wait_recv)
        when_owner(rank, print_copy(p).wait_send)

    @pl.loop(groups - 1 - late, groups - 1)
    def _(k):
        block_copy(k).wait_recv()

    @pl.loop(1, groups - 1)
    def _(k):
        block_copy(k).wait_send()


def place(n_section, n_tensor, layers, late,
          order_ref, late_probes, blocks_ref, sums_ref, print_ref, means_ref,
          weights_out, sums_out, print_out, means_out,
          total, block_sem, mean_sem, sum_sem, print_sem):
    section, tensor = (lax.axis_index(a) for a in ("section", "tensor"))
    groups = blocks_ref.shape[0]
    per_layer = groups // layers
    chunk = sums_ref.shape[0] // sum_sem.shape[0]
    order = [jnp.max(order_ref[b:b + 1, :]).astype(jnp.int32) for b in range(layers)]

    def copies(b):
        at, to = pl.ds(b * per_layer, per_layer), pl.ds(order[b] * per_layer, per_layer)
        return (pltpu.make_async_copy(blocks_ref.at[at], weights_out.at[to], block_sem.at[b]),
                pltpu.make_async_copy(means_ref.at[at], means_out.at[to], mean_sem.at[b]))

    def sum_copy(r):
        at = pl.ds(r * chunk, chunk)
        return pltpu.make_async_copy(total.at[at], sums_out.at[at], sum_sem.at[r])

    print_copy = pltpu.make_async_copy(print_ref, print_out, print_sem)

    for b in range(layers):
        for copy in copies(b):
            copy.start()
    print_copy.start()

    for r in range(sum_sem.shape[0]):
        at = slice(r * chunk, (r + 1) * chunk)
        value = sums_ref[at, :]
        for j in range(late):
            s, t = partner_of(n_section, n_tensor, section, tensor, groups - 1 - late + j, -1)
            value += jnp.dot(late_probes[j, at, :], blocks_ref[s * n_tensor + t],
                             preferred_element_type=jnp.float32)
        total[at, :] = value
        sum_copy(r).start()

    for b in range(layers):
        for copy in copies(b):
            copy.wait()
    print_copy.wait()
    for r in range(sum_sem.shape[0]):
        sum_copy(r).wait()


def local(n_section, n_expert, n_tensor, branch_weights, branch_gains, column_order,
          layer_order, probe_seeds):
    _, rows, width = branch_weights.shape
    groups = n_section * n_tensor
    cols = width // groups
    layers = layer_order.shape[0]
    n_probes = probe_seeds.shape[0]
    deep = min(1024, width)
    late = min(LATE, groups - 2)
    n_tall = 2 if rows % 32 == 0 else 1
    n_pieces = n_tall * len(column_spans(cols))
    near = n_section * halves(n_tensor)[0]
    owners = near if n_probes % (128 * near) == 0 else min(near, n_probes // 128)
    f32, bf16 = jnp.float32, jnp.bfloat16
    vmem = pl.BlockSpec(memory_space=pltpu.VMEM)
    hbm = pl.BlockSpec(memory_space=pltpu.HBM)
    dma = pltpu.SemaphoreType.DMA
    arrived, sums, printed, means, late_probes, order = pl.pallas_call(
        functools.partial(exchange, n_section, n_expert, n_tensor, layers, late),
        out_shape=(
            jax.ShapeDtypeStruct((groups, rows, cols), bf16),
            jax.ShapeDtypeStruct((n_probes, cols), f32),
            jax.ShapeDtypeStruct((1, n_probes), f32),
            jax.ShapeDtypeStruct((groups, 1, rows), f32),
            jax.ShapeDtypeStruct((late, n_probes, rows), bf16),
            jax.ShapeDtypeStruct((-(-layers // 8) * 8, 128), f32),
        ),
        in_specs=[hbm] * 5,
        out_specs=(vmem,) * 6,
        scratch_shapes=[
            pltpu.VMEM((rows, width), bf16),
            pltpu.VMEM((groups, rows, cols), bf16),
            pltpu.VMEM((rows, cols), f32),
            pltpu.VMEM((width, cols), bf16),
            pltpu.VMEM((rows, 128), f32),
            pltpu.VMEM((rows, 128), f32),
            pltpu.VMEM((n_probes, 128), jnp.int32),
            pltpu.VMEM((n_probes, rows), bf16),
            pltpu.VMEM((n_expert, 1, rows), f32),
            pltpu.VMEM((groups, 1, n_probes // owners), f32),
            pltpu.VMEM((1, n_probes), f32),
            pltpu.VMEM((1, width), jnp.int32),
            pltpu.VMEM((1, n_probes), jnp.int32),
            pltpu.SMEM((1, layers), jnp.int32),
            pltpu.VMEM((1, rows), f32),
            pltpu.VMEM((1, rows), f32),
            dma((n_tall, width // deep)), dma((groups,)), dma((groups,)),
            dma((n_expert,)), dma((n_expert,)), dma((2 * near,)), dma((2 * near,)),
            dma((groups,)), dma((groups,)), dma((near,)), dma((near,)),
            dma((n_pieces,)), dma((n_pieces,)), dma((2,)), dma((4,)),
        ],
        compiler_params=pltpu.CompilerParams(
            collective_id=0, has_side_effects=True, vmem_limit_bytes=40 * 2 ** 20),
        name="exchange",
    )(*(pltpu.with_memory_space_constraint(x, pltpu.HBM) for x in (
        layer_order.reshape(1, layers), branch_weights, branch_gains, column_order,
        probe_seeds.reshape(1, n_probes))))

    n_sums = 2 if n_probes % 512 == 0 else 1
    weights, sums, printed, means = pl.pallas_call(
        functools.partial(place, n_section, n_tensor, layers, late),
        in_specs=[vmem] * 6,
        out_specs=(hbm, hbm, hbm, hbm),
        scratch_shapes=[
            pltpu.VMEM((n_probes, cols), f32), dma((layers,)), dma((layers,)), dma((n_sums,)),
            dma(())],
        out_shape=(
            jax.ShapeDtypeStruct((groups, rows, cols), bf16),
            jax.ShapeDtypeStruct((n_probes, cols), f32),
            jax.ShapeDtypeStruct((1, n_probes), f32),
            jax.ShapeDtypeStruct((groups, 1, rows), f32),
        ),
        compiler_params=pltpu.CompilerParams(
            has_side_effects=True, vmem_limit_bytes=16 * 2 ** 20),
        name="place",
    )(order, late_probes, arrived, sums, printed, means)
    return (weights.reshape(1, groups * rows, cols), sums[None], printed,
            means.reshape(groups * rows))


def solution(mesh):
    sizes = mesh.shape
    return jax.shard_map(
        functools.partial(local, sizes["section"], sizes["expert"], sizes["tensor"]),
        mesh=mesh,
        in_specs=(
            P("expert", ("section", "tensor"), None),
            P("expert", ("section", "tensor")),
            P("expert", None),
            P(),
            P(),
        ),
        out_specs=(
            P("expert", None, ("section", "tensor")),
            P("expert", None, ("section", "tensor")),
            P("expert", None),
            P(),
        ),
        check_vma=False,
    )
```
